32 devices in a mesh: tm: 4 (over y, x), space: 8 (over z, core).
Axes of the slice: x: 2, y: 2, z: 4, core: 2. Of those that a mesh axis runs over, the one named last changes fastest.
Arguments:
- initial_state: float32 [3, 192, 256], P(None, 'space'), may hold values from -2 to 2
- c_guess: float32 [4, 3, 192, 256], P('tm', None, 'space'), may hold values from -2 to 2
- friction: float32 [192, 256], P('space'), may hold values from 0.05 to 1
Outputs:
- c_points: float32 [4, 3, 192, 256], P('tm', None, 'space')
- f_points: float32 [4, 3, 192, 256], P('tm', None, 'space')
The draws below stay inside these ranges and needn't reach their ends.
All inputs are finite; a program needn't handle non-finite values.
Results may differ from the reference program's by a relative error of at most 0.00012.
Values sent between devices are 32-bit elements; how exact they have to be, the bound alone decides.
No kernel may reach another device: no remote copies, remote signals or barrier semaphores. Data moves between devices by JAX's collectives and lax.ppermute only.
A program may use at most 64 MiB of HBM per device.

```python
import math
import jax
import jax.numpy as jnp
from jax import lax

NY = 256
STEPS = 8
NT = 4
NX = 192


def block_levels(rng, dims, shards, low, high):
    gain, own = 1.0, jax.random.fold_in(rng, 6)
    for dim, parts in shards:
        heights = jnp.exp(jax.random.uniform(jax.random.fold_in(own, dim), (parts,), jnp.float32, low / len(shards), high / len(shards)))
        gain = gain * jnp.repeat(heights, dims[dim] // parts).reshape([-1 if axis == dim else 1 for axis in range(len(dims))])
    return gain


def scatter_about(rng, shape, deviation, bound, pieces=(), kind=jnp.bfloat16):
    values = deviation * jax.random.normal(rng, shape, jnp.float32)
    if pieces:
        values = values * block_levels(rng, shape, pieces, -0.22, 0.18)
    return jnp.clip(values, -bound, bound).astype(kind)


def setup_inputs(seed: int = 0) -> dict:
    streams_of = jax.random.split(jax.random.key(seed), 4)
    initial_state = scatter_about(streams_of[0], (3, NX, NY), 0.15, 2.0, ((1, 8),), jnp.float32)
    c_guess = scatter_about(streams_of[1], (NT, 3, NX, NY), 0.15, 2.0, ((0, 4), (2, 8)), jnp.float32)
    friction = jnp.clip(jnp.exp(math.log(1.0) - 2.9957323 * jax.random.uniform(streams_of[2], (NX, NY), jnp.float32) ** block_levels(streams_of[2], (NX, NY), ((0, 8),), -0.2, 0.2)), 0.05, 1.0)
    return {"initial_state": initial_state, "c_guess": c_guess, "friction": friction}


gravity = 2.0
coriolis = 0.5
viscosity = 0.5
time_step = 0.04


def roll_neighbours(field):
    return (jnp.roll(field, -1, 0), jnp.roll(field, 1, 0), jnp.roll(field, -1, 1), jnp.roll(field, 1, 1), field)


def spread(near):
    return near[0] + near[1] + near[2] + near[3] - 4.0 * near[4]


def tendency(fields, drag, neighbours):
    height = fields[0]
    row_vel = fields[1]
    col_vel = fields[2]
    height_near = neighbours(height)
    row_near = neighbours(row_vel)
    col_near = neighbours(col_vel)
    flux_row = neighbours((1.0 + height) * row_vel)
    flux_col = neighbours((1.0 + height) * col_vel)
    row_mid = row_near[4]
    col_mid = col_near[4]
    rate_height = -(0.5 * (flux_row[0] - flux_row[1]) + 0.5 * (flux_col[2] - flux_col[3])) + viscosity * spread(height_near)
    rate_row = (-(row_mid * (0.5 * (row_near[0] - row_near[1])) + col_mid * (0.5 * (row_near[2] - row_near[3])))
                - gravity * (0.5 * (height_near[0] - height_near[1])) + coriolis * col_mid - drag * row_mid
                + viscosity * spread(row_near))
    rate_col = (-(row_mid * (0.5 * (col_near[0] - col_near[1])) + col_mid * (0.5 * (col_near[2] - col_near[3])))
                - gravity * (0.5 * (height_near[2] - height_near[3])) - coriolis * row_mid - drag * col_mid
                + viscosity * spread(col_near))
    return jnp.stack([rate_height, rate_row, rate_col])


def heun_step(fields, drag, size):
    slope_one = tendency(fields, drag, roll_neighbours)
    midpoint = fields + size * slope_one
    slope_two = tendency(midpoint, drag, roll_neighbours)
    return fields + (0.5 * size) * (slope_one + slope_two)


def reference(initial_state, c_guess, friction):
    coarse_step = STEPS * time_step

    def advance(fields, step_count):
        def inner(turn, moving):
            return heun_step(moving, friction, time_step)
        return lax.fori_loop(0, step_count, inner, fields)

    def earlier(stack):
        return jnp.concatenate([initial_state[None], stack[:-1]], 0)

    relaxed = lax.map(lambda fields: advance(fields, STEPS), earlier(c_guess))
    defect = lax.map(lambda fields: advance(fields, STEPS) - heun_step(fields, friction, coarse_step), earlier(relaxed))

    def chain(carried, defect_now):
        result = heun_step(carried, friction, coarse_step) + defect_now
        return result, result

    unused, c_points = lax.scan(chain, initial_state, defect)
    f_points = lax.map(lambda fields: advance(fields, STEPS - 1), earlier(c_points))
    return c_points, f_points
```

```python
import jax
import jax.numpy as jnp
from jax import lax
from jax.experimental import pallas as pl
from jax.experimental.pallas import tpu as pltpu
from jax.sharding import PartitionSpec as P

STEPS = 8


gravity = 2.0
coriolis = 0.5
viscosity = 0.5
time_step = 0.04

LANES = 128
BLOCK = 8
VMEM = pl.BlockSpec(memory_space=pltpu.VMEM)
SMEM = pl.BlockSpec(memory_space=pltpu.SMEM)


def across(tiles):
    count = len(tiles)
    lane = lax.broadcasted_iota(jnp.int32, tiles[0].shape, 1)
    up = [pltpu.roll(tile, LANES - 1, 1) for tile in tiles]
    down = [pltpu.roll(tile, 1, 1) for tile in tiles]
    east = [jnp.where(lane == LANES - 1, up[(i + 1) % count], up[i]) for i in range(count)]
    west = [jnp.where(lane == 0, down[i - 1], down[i]) for i in range(count)]
    return east, west


def slopes(src, row, tiles):
    here = [[src[f, i, pl.ds(row, BLOCK), :] for i in range(tiles)] for f in range(3)]
    north = [[src[f, i, pl.ds(row + 1, BLOCK), :] for i in range(tiles)] for f in range(3)]
    south = [[src[f, i, pl.ds(row - 1, BLOCK), :] for i in range(tiles)] for f in range(3)]
    sides = [across(here[f]) for f in range(3)]
    out = []
    for i in range(tiles):
        u, w = here[1][i], here[2][i]
        en, un, wn = (north[f][i] for f in range(3))
        es, us, ws = (south[f][i] for f in range(3))
        ee, ue, we = (sides[f][0][i] for f in range(3))
        ew, uw, ww = (sides[f][1][i] for f in range(3))
        un_us, we_ww = un - us, we - ww
        rest_e = (en * (1.0 - un) + es * (1.0 + us)) + (ee * (1.0 - we) + ew * (1.0 + ww))
        rest_e = (rest_e - un_us) - we_ww
        rest_u = ((un + us) - u * un_us) + ((ue + uw) - w * (ue - uw))
        rest_w = ((wn + ws) - u * (wn - ws)) + ((we + ww) - w * we_ww)
        rest_u = rest_u + ((2.0 * coriolis) * w - (2.0 * gravity * 0.5) * (en - es))
        rest_w = rest_w - ((2.0 * coriolis) * u + (2.0 * gravity * 0.5) * (ee - ew))
        out.append((rest_e, rest_u, rest_w))
    return here, out


def own_factor(keep, i, row, size):
    kept = keep[i, pl.ds(row, BLOCK), :]
    ratio = size / time_step
    return kept if ratio == 1.0 else ratio * kept + (1.0 - ratio)


def first_stage(src, mid, keep, blocks, pad, size, tiles):
    for block in blocks:
        row = pad + BLOCK * block
        here, rest = slopes(src, row, tiles)
        for i in range(tiles):
            factor = own_factor(keep, i, row, size)
            for f in range(3):
                own = (1.0 - 2.0 * size) if f == 0 else factor
                mid[f, i, pl.ds(row, BLOCK), :] = own * here[f][i] + (0.5 * size) * rest[i][f]


def second_stage(src, mid, keep, blocks, pad, size, tiles, put):
    for block in blocks:
        row = pad + BLOCK * block
        here, rest = slopes(mid, row, tiles)
        for i in range(tiles):
            factor = own_factor(keep, i, row, size)
            for f in range(3):
                own = (1.0 - 2.0 * size) if f == 0 else factor
                old = src[f, i, pl.ds(row, BLOCK), :]
                new = 0.5 * ((old + own * here[f][i]) + (0.5 * size) * rest[i][f])
                put(block, f, i, old, new)


def fine_kernel(layout, which_ref, *refs):
    count, strip, margin, tiles, slices = layout
    parts = refs[: 2 * count + 1]
    narrow_ref, far_ref, wide_ref, state, mid, keep, before, coarse = refs[2 * count + 1 :]
    rows = (2 * count + 1) * strip
    pad = BLOCK
    centre = count * strip // BLOCK
    strip_blocks = range(centre, centre + strip // BLOCK)
    total = rows // BLOCK
    reach = 4 * STEPS
    which = which_ref[0]

    for ref in (state, mid):
        for f in range(3):
            for i in range(tiles):
                for row in (0, pad + rows):
                    ref[f, i, pl.ds(row, BLOCK), :] = jnp.zeros((BLOCK, LANES), jnp.float32)
    for p, part in enumerate(parts):
        for b in range(strip // BLOCK):
            row = pad + p * strip + b * BLOCK
            for i in range(tiles):
                columns = pl.ds(i * LANES, LANES)
                for f in range(3):
                    state[f, i, pl.ds(row, BLOCK), :] = part[f, pl.ds(b * BLOCK, BLOCK), columns]
                drag = part[3, pl.ds(b * BLOCK, BLOCK), columns]
                keep[i, pl.ds(row, BLOCK), :] = (1.0 - 2.0 * time_step) - time_step * drag

    def put(block, f, i, old, new):
        if block in strip_blocks:
            before[f, i, pl.ds((block - centre) * BLOCK, BLOCK), :] = old
        state[f, i, pl.ds(pad + BLOCK * block, BLOCK), :] = new

    def steps(start, group):
        first, last = start // BLOCK, total - start // BLOCK

        def one(turn, carry):
            first_stage(state, mid, keep, range(first, last), pad, time_step, tiles)
            second_stage(state, mid, keep, range(first, last), pad, time_step, tiles, put)
            return carry

        lax.fori_loop(0, group, one, 0)

    def emit(target, source, rows_from, row_count):
        for f in range(3):
            for i in range(tiles):
                for b in range(0, row_count, BLOCK):
                    take = min(BLOCK, row_count - b)
                    target[f, pl.ds(b, take), pl.ds(i * LANES, LANES)] = source(f, i, rows_from + b, take)

    def from_state(f, i, row, take):
        return state[f, i, pl.ds(pad + row, take), :]

    def from_before(f, i, row, take):
        return before[f, i, pl.ds(row, take), :]

    group = BLOCK // 2
    for start in range(0, STEPS, group):
        steps(2 * start, group)

    edge = count * strip - margin
    out_first, out_last = edge // BLOCK, (edge + strip + 2 * margin) // BLOCK

    @pl.when(which == slices - 2)
    def _():
        emit(narrow_ref, from_state, count * strip, strip)
        emit(far_ref, from_before, 0, strip)

    def put_coarse(block, f, i, old, new):
        coarse[f, i, pl.ds((block - out_first) * BLOCK, BLOCK), :] = new

    size = STEPS * time_step
    first_stage(state, mid, keep, range(out_first - 1, out_last + 1), pad, size, tiles)
    second_stage(state, mid, keep, range(out_first, out_last), pad, size, tiles, put_coarse)

    for start in range(STEPS, 2 * STEPS, group):
        steps(2 * start, group)

    def from_defect(f, i, row, take):
        return state[f, i, pl.ds(pad + row, take), :] - coarse[f, i, pl.ds(row - edge, take), :]

    wide = strip + 2 * margin

    @pl.when(which < slices - 2)
    def _():
        emit(narrow_ref, from_defect, count * strip, strip)
        emit(far_ref, from_defect, edge + 2, wide - 4)
        emit(wide_ref, from_defect, edge, wide)

    @pl.when(which >= slices - 2)
    def _():
        emit(wide_ref, from_state, edge, wide)

    @pl.when(which == slices - 1)
    def _():
        emit(narrow_ref, from_state, count * strip, strip)
        emit(far_ref, from_before, 0, strip)


def fine_chain(which, parts, margin, slices):
    count = len(parts) // 2
    strip, columns = parts[0].shape[1:]
    tiles = columns // LANES
    wide = strip + 2 * margin
    rows = len(parts) * strip + 2 * BLOCK
    shape = lambda n: jax.ShapeDtypeStruct((3, n, columns), jnp.float32)
    layout = (count, strip, margin, tiles, slices)
    return pl.pallas_call(
        lambda *refs: fine_kernel(layout, *refs),
        name="fine_chain",
        out_shape=(shape(strip), shape(wide - 4), shape(wide)),
        in_specs=[SMEM] + [VMEM] * len(parts),
        out_specs=(VMEM, VMEM, VMEM),
        scratch_shapes=[
            pltpu.VMEM((3, tiles, rows, LANES), jnp.float32),
            pltpu.VMEM((3, tiles, rows, LANES), jnp.float32),
            pltpu.VMEM((tiles, rows, LANES), jnp.float32),
            pltpu.VMEM((3, tiles, strip, LANES), jnp.float32),
            pltpu.VMEM((3, tiles, wide, LANES), jnp.float32),
        ],
    )(which, *parts)


def last_kernel(layout, which_ref, wide_ref, defects_ref, narrow_ref, far_ref, *refs):
    strip, margin, tiles, drag_from, count = layout
    drags = refs[:count]
    c_ref, f_ref, state, mid, keep = refs[count:]
    wide = strip + 2 * margin
    pad = BLOCK
    which = which_ref[0]
    total = wide // BLOCK
    chain = defects_ref.shape[0]

    for ref in (state, mid):
        for f in range(3):
            for i in range(tiles):
                for row in (0, pad + wide):
                    ref[f, i, pl.ds(row, BLOCK), :] = jnp.zeros((BLOCK, LANES), jnp.float32)
    for b in range(total):
        at = drag_from + b * BLOCK
        part = drags[at // strip]
        for i in range(tiles):
            columns = pl.ds(i * LANES, LANES)
            drag = part[3, pl.ds(at % strip, BLOCK), columns]
            keep[i, pl.ds(pad + b * BLOCK, BLOCK), :] = (1.0 - 2.0 * time_step) - time_step * drag
            for f in range(3):
                state[f, i, pl.ds(pad + b * BLOCK, BLOCK), :] = wide_ref[f, pl.ds(b * BLOCK, BLOCK), columns]

    coarse_size = STEPS * time_step

    def put(block, f, i, old, new):
        state[f, i, pl.ds(pad + BLOCK * block, BLOCK), :] = new

    def link(turn):
        first_stage(state, mid, keep, range(total), pad, coarse_size, tiles)
        second_stage(state, mid, keep, range(total), pad, coarse_size, tiles, put)
        for f in range(3):
            for i in range(tiles):
                for b in range(0, wide - 4, BLOCK):
                    take = min(BLOCK, wide - 4 - b)
                    add = defects_ref[turn, f, pl.ds(b, take), pl.ds(i * LANES, LANES)]
                    at = pl.ds(pad + 2 + b, take)
                    state[f, i, at, :] = state[f, i, at, :] + add

    for turn in range(chain):
        pl.when(which > turn + 2)(lambda: link(turn))

    first = margin // BLOCK
    strip_blocks = range(first, first + strip // BLOCK)

    def put_c(block, f, i, old, new):
        b = (block - first) * BLOCK
        columns = pl.ds(i * LANES, LANES)
        value = narrow_ref[f, pl.ds(b, BLOCK), columns]
        c_ref[f, pl.ds(b, BLOCK), columns] = jnp.where(which < 2, value, new + value)

    def put_f(block, f, i, old, new):
        b = (block - first) * BLOCK
        columns = pl.ds(i * LANES, LANES)
        value = far_ref[f, pl.ds(b, BLOCK), columns]
        f_ref[f, pl.ds(b, BLOCK), columns] = jnp.where(which < 2, value, new)

    first_stage(state, mid, keep, range(first - 1, first + strip // BLOCK + 1), pad, coarse_size, tiles)
    second_stage(state, mid, keep, strip_blocks, pad, coarse_size, tiles, put_c)

    def one(turn, carry):
        first_stage(state, mid, keep, range(total), pad, time_step, tiles)
        second_stage(state, mid, keep, range(total), pad, time_step, tiles, put)
        return carry

    lax.fori_loop(0, STEPS - 2, one, 0)
    first_stage(state, mid, keep, range(first - 1, first + strip // BLOCK + 1), pad, time_step, tiles)
    second_stage(state, mid, keep, strip_blocks, pad, time_step, tiles, put_f)


def last_chain(which, wide, defects, narrow, far, parts, margin):
    strip, columns = narrow.shape[1:]
    tiles = columns // LANES
    rows = strip + 2 * margin + 2 * BLOCK
    count = len(parts)
    layout = (strip, margin, tiles, (count // 2) * strip - margin, count)
    shape = jax.ShapeDtypeStruct((3, strip, columns), jnp.float32)
    return pl.pallas_call(
        lambda *refs: last_kernel(layout, *refs),
        name="last_chain",
        out_shape=(shape, shape),
        in_specs=[SMEM] + [VMEM] * (4 + count),
        out_specs=(VMEM, VMEM),
        scratch_shapes=[
            pltpu.VMEM((3, tiles, rows, LANES), jnp.float32),
            pltpu.VMEM((3, tiles, rows, LANES), jnp.float32),
            pltpu.VMEM((tiles, rows, LANES), jnp.float32),
        ],
    )(which, wide, defects, narrow, far, *parts)


def body(initial_state, c_guess, friction):
    slices, strips = lax.axis_size("tm"), lax.axis_size("space")
    strip = initial_state.shape[1]
    which = lax.axis_index("tm")
    margin = 2 * (STEPS - 1) + 2 * (slices - 3)
    count = -(-(4 * STEPS + margin) // strip)
    both = ("tm", "space")

    def moved(value, target):
        pairs = []
        for t in range(slices):
            for s in range(strips):
                to = target(t, s)
                if to is not None:
                    pairs.append((t * strips + s, to[0] * strips + to[1] % strips))
        return lax.ppermute(value, both, pairs)

    start = jnp.where(which >= slices - 2, initial_state, c_guess[0])
    own = jnp.concatenate([start, friction[None]], axis=0)
    parts = []
    for offset in range(-count, count + 1):
        parts.append(own if offset == 0 else moved(own, lambda t, s, o=offset: (t, s - o)))
    index = which.astype(jnp.int32).reshape(1)
    narrow, far, wide = fine_chain(index, parts, margin, slices)

    got = moved(narrow, lambda t, s: ((t + 2) % slices, s))
    lasts = {slices - 2: 0, slices - 1: 1}
    if slices == 4:
        lasts[0] = slices - 1
    got_far = moved(far, lambda t, s: (lasts[t], s) if t in lasts else None)
    if slices == 4:
        defects = got_far[None]
    else:
        everyone = lax.all_gather(wide, "tm", axis=0)
        defects = everyone[: slices - 3, :, 2:-2]
        wide = everyone[slices - 1]
    c_points, f_points = last_chain(index, wide, defects, got, got_far, parts, margin)
    return (c_points[None], f_points[None])


def solution(mesh):
    placed = (P(None, "space", None), P("tm", None, "space", None), P("space", None))
    return jax.shard_map(
        body,
        mesh=mesh,
        in_specs=placed,
        out_specs=(P("tm", None, "space", None), P("tm", None, "space", None)),
        check_vma=False,
    )
```

```python
import jax
import jax.numpy as jnp
from jax import lax
from jax.experimental import pallas as pl
from jax.experimental.pallas import tpu as pltpu
from jax.sharding import PartitionSpec as P

STEPS = 8


gravity = 2.0
coriolis = 0.5
viscosity = 0.5
time_step = 0.04

LANES = 128
BLOCK = 8
VMEM = pl.BlockSpec(memory_space=pltpu.VMEM)
SMEM = pl.BlockSpec(memory_space=pltpu.SMEM)
VMEM_LIMIT = 8 * 2**20
FLOPS_PER_US = 500_000_000


def lanes():
    return lax.broadcasted_iota(jnp.int32, (BLOCK, LANES), 1)


def pick(tile, index):
    return jnp.take_along_axis(tile, index, axis=1, mode="promise_in_bounds")


def dealt(natural):
    tiles = len(natural)
    out = []
    for i in range(tiles):
        column = tiles * lanes() + i
        index = lax.rem(column, LANES)
        value = pick(natural[0], index)
        for p in range(1, tiles):
            value = jnp.where(column >= p * LANES, pick(natural[p], index), value)
        out.append(value)
    return out


def gathered(tiled):
    tiles = len(tiled)
    out = []
    for p in range(tiles):
        column = p * LANES + lanes()
        index = column // tiles
        which = lax.rem(column, tiles)
        value = pick(tiled[0], index)
        for i in range(1, tiles):
            value = jnp.where(which == i, pick(tiled[i], index), value)
        out.append(value)
    return out


def east(tiled):
    return tiled[1:] + [pltpu.roll(tiled[0], LANES - 1, 1)]


def west(tiled):
    return [pltpu.roll(tiled[-1], 1, 1)] + tiled[:-1]


def slopes(src, row, tiles):
    def rows(plane, by):
        return [src[plane, i, pl.ds(row + by, BLOCK), :] for i in range(tiles)]

    here = [rows(f, 0) for f in range(3)]
    north = [rows(f, 1) for f in range(4)]
    south = [rows(f, -1) for f in range(4)]
    flux = rows(4, 0)
    easts = [east(value) for value in here + [flux]]
    wests = [west(value) for value in here + [flux]]
    out = []
    for i in range(tiles):
        u, w = here[1][i], here[2][i]
        en, un, wn, fn = (north[f][i] for f in range(4))
        es, us, ws, fs = (south[f][i] for f in range(4))
        ee, ue, we, ge = (easts[f][i] for f in range(4))
        ew, uw, ww, gw = (wests[f][i] for f in range(4))
        rest_e = ((en + es) + (ee + ew)) - ((fn - fs) + (ge - gw))
        rest_u = ((un + us) - u * (un - us)) + ((ue + uw) - w * (ue - uw))
        rest_w = ((wn + ws) - u * (wn - ws)) + ((we + ww) - w * (we - ww))
        rest_u = rest_u + (w - (en - es))
        rest_w = rest_w - (u + (ee - ew))
        out.append((rest_e, rest_u, rest_w))
    return here, out


def own_factor(keep, i, row, size):
    kept = keep[i, pl.ds(row, BLOCK), :]
    ratio = size / time_step
    return kept if ratio == 1.0 else ratio * kept + (1.0 - ratio)


def store(ref, i, row, value):
    at = pl.ds(row, BLOCK)
    for f in range(3):
        ref[f, i, at, :] = value[f]
    height = 2.0 + value[0]
    ref[3, i, at, :] = height * value[1]
    ref[4, i, at, :] = height * value[2]


def first_stage(src, mid, keep, blocks, pad, size, tiles):
    for block in blocks:
        row = pad + BLOCK * block
        here, rest = slopes(src, row, tiles)
        for i in range(tiles):
            factor = own_factor(keep, i, row, size)
            value = []
            for f in range(3):
                own = (1.0 - 2.0 * size) if f == 0 else factor
                value.append(own * here[f][i] + (0.5 * size) * rest[i][f])
            store(mid, i, row, value)


def second_stage(src, mid, keep, blocks, pad, size, tiles, put):
    for block in blocks:
        row = pad + BLOCK * block
        here, rest = slopes(mid, row, tiles)
        for i in range(tiles):
            factor = own_factor(keep, i, row, size)
            olds, news = [], []
            for f in range(3):
                own = (1.0 - 2.0 * size) if f == 0 else factor
                old = src[f, i, pl.ds(row, BLOCK), :]
                olds.append(old)
                news.append(0.5 * ((old + own * here[f][i]) + (0.5 * size) * rest[i][f]))
            put(block, i, olds, news)


def clear(ref, planes, tiles, starts):
    for f in range(planes):
        for i in range(tiles):
            for row in starts:
                ref[f, i, pl.ds(row, BLOCK), :] = jnp.zeros((BLOCK, LANES), jnp.float32)


def copy_rows(target, source, tiles, row_count, to, start):
    for f in range(3):
        for i in range(tiles):
            for b in range(0, row_count, BLOCK):
                take = min(BLOCK, row_count - b)
                target[f, i, pl.ds(to + b, take), :] = source(f, i, start + b, take)


def copy_natural(target, source, tiles, row_count, start):
    for f in range(3):
        for b in range(0, row_count, BLOCK):
            tiled = [source(f, i, start + b, BLOCK) for i in range(tiles)]
            for p, value in enumerate(gathered(tiled)):
                target[f, pl.ds(b, BLOCK), pl.ds(p * LANES, LANES)] = 0.5 * value if f == 0 else value


def fine_kernel(layout, which_ref, *refs):
    count, strip, margin, tiles, slices, paired = layout
    parts = refs[: 2 * count + 1]
    narrow_ref, far_ref, wide_ref, factor_ref, state, mid, keep, before, coarse = refs[2 * count + 1 :]
    rows = (2 * count + 1) * strip
    pad = BLOCK
    centre = count * strip // BLOCK
    strip_blocks = range(centre, centre + strip // BLOCK)
    total = rows // BLOCK
    which = which_ref[0]

    for ref in (state, mid):
        clear(ref, 5, tiles, (0, pad + rows))

    def load(p, part):
        for b in range(0, strip, BLOCK):
            row = pad + p * strip + b
            if not isinstance(p, int):
                row = pl.multiple_of(row, BLOCK)
            if len(part.shape) == 4:
                planes = [[part[f, i, pl.ds(b, BLOCK), :] for i in range(tiles)] for f in range(4)]
            else:
                planes = dealt_block(part, b, tiles)
            for i in range(tiles):
                store(state, i, row, [planes[f][i] for f in range(3)])
                keep[i, pl.ds(row, BLOCK), :] = planes[3][i]

    for p, part in enumerate(parts):
        load(which_ref[1 + p] if paired and p != count else p, part)

    def put(block, i, olds, news):
        if block in strip_blocks:
            for f in range(3):
                before[f, i, pl.ds((block - centre) * BLOCK, BLOCK), :] = olds[f]
        store(state, i, pad + BLOCK * block, news)

    def steps(start, group):
        first, last = start // BLOCK, total - start // BLOCK

        def one(turn, carry):
            first_stage(state, mid, keep, range(first, last), pad, time_step, tiles)
            second_stage(state, mid, keep, range(first, last), pad, time_step, tiles, put)
            return carry

        lax.fori_loop(0, group, one, 0)

    def from_state(f, i, row, take):
        return state[f, i, pl.ds(pad + row, take), :]

    def from_before(f, i, row, take):
        return before[f, i, pl.ds(row, take), :]

    group = BLOCK // 2
    for start in range(0, STEPS, group):
        steps(2 * start, group)

    wide = strip + 2 * margin
    edge = count * strip - margin
    out_first, out_last = edge // BLOCK, (edge + wide) // BLOCK

    @pl.when(which == slices - 2)
    def _():
        copy_natural(narrow_ref, from_state, tiles, strip, count * strip)

    @pl.when(which == slices - 1)
    def _():
        copy_rows(far_ref, from_before, tiles, strip, 0, 0)

    def put_coarse(block, i, olds, news):
        for f in range(3):
            coarse[f, i, pl.ds((block - out_first) * BLOCK, BLOCK), :] = news[f]

    size = STEPS * time_step
    first_stage(state, mid, keep, range(out_first - 1, out_last + 1), pad, size, tiles)
    second_stage(state, mid, keep, range(out_first, out_last), pad, size, tiles, put_coarse)

    for start in range(STEPS, 2 * STEPS, group):
        steps(2 * start, group)

    def from_defect(f, i, row, take):
        return state[f, i, pl.ds(pad + row, take), :] - coarse[f, i, pl.ds(row - edge, take), :]

    for i in range(tiles):
        for b in range(0, wide + 2 * pad, BLOCK):
            factor_ref[i, pl.ds(b, BLOCK), :] = keep[i, pl.ds(edge + b, BLOCK), :]

    @pl.when(which < slices - 2)
    def _():
        copy_natural(narrow_ref, from_defect, tiles, strip, count * strip)
        copy_rows(far_ref, from_defect, tiles, wide - 4, 0, edge + 2)
        copy_rows(wide_ref, from_defect, tiles, wide, 0, edge)

    @pl.when(which >= slices - 2)
    def _():
        copy_rows(wide_ref, from_state, tiles, wide, 0, edge)

    @pl.when(which == slices - 2)
    def _():
        copy_rows(far_ref, from_before, tiles, strip, 0, 0)

    @pl.when(which == slices - 1)
    def _():
        copy_natural(narrow_ref, from_state, tiles, strip, count * strip)


def array(*shape):
    return jax.ShapeDtypeStruct(shape, jnp.float32)


def scratch(*shape):
    return pltpu.VMEM(shape, jnp.float32)


def call(kernel, name, micros, out_shape, args, scratches=()):
    return pl.pallas_call(
        kernel,
        name=name,
        out_shape=out_shape,
        in_specs=[SMEM] + [VMEM] * (len(args) - 1),
        out_specs=tuple(VMEM for _ in out_shape),
        scratch_shapes=list(scratches),
        compiler_params=pltpu.CompilerParams(vmem_limit_bytes=VMEM_LIMIT),
        cost_estimate=pl.CostEstimate(flops=int(micros * FLOPS_PER_US), bytes_accessed=0, transcendentals=0),
    )(*args)


def dealt_block(ref, b, tiles):
    out = []
    for f in range(4):
        tiled = dealt([ref[f, pl.ds(b, BLOCK), pl.ds(p * LANES, LANES)] for p in range(tiles)])
        if f == 0:
            tiled = [2.0 * value for value in tiled]
        if f == 3:
            tiled = [(1.0 - 2.0 * time_step) - time_step * value for value in tiled]
        out.append(tiled)
    return out


def deal_kernel(tiles, which_ref, *refs):
    half = len(refs) // 2
    for ref, out_ref in zip(refs[:half], refs[half:]):
        for b in range(0, ref.shape[1], BLOCK):
            for f, tiled in enumerate(dealt_block(ref, b, tiles)):
                for i, value in enumerate(tiled):
                    out_ref[f, i, pl.ds(b, BLOCK), :] = value


def deal(which, *parts):
    strip, columns = parts[0].shape[1:]
    tiles = columns // LANES
    out = tuple(array(4, tiles, strip, LANES) for _ in parts)
    return call(lambda *refs: deal_kernel(tiles, *refs), "deal", 0.5, out, [which, *parts])


def fine_chain(which, parts, margin, slices, paired):
    count = len(parts) // 2
    tiles, strip = parts[0].shape[1:3]
    wide = strip + 2 * margin
    rows = len(parts) * strip + 2 * BLOCK
    layout = (count, strip, margin, tiles, slices, paired)
    return call(
        lambda *refs: fine_kernel(layout, *refs),
        "fine_chain",
        8,
        (
            array(3, strip, tiles * LANES),
            array(3, tiles, wide - 4, LANES),
            array(3, tiles, wide, LANES),
            array(tiles, wide + 2 * BLOCK, LANES),
        ),
        [which, *parts],
        [
            scratch(5, tiles, rows, LANES),
            scratch(5, tiles, rows, LANES),
            scratch(tiles, rows, LANES),
            scratch(3, tiles, strip, LANES),
            scratch(3, tiles, wide, LANES),
        ],
    )


def widen(state, wide_ref, wide, tiles, pad):
    clear(state, 5, tiles, (0, pad + wide))
    for i in range(tiles):
        for b in range(0, wide, BLOCK):
            store(state, i, pad + b, [wide_ref[f, i, pl.ds(b, BLOCK), :] for f in range(3)])


def link_kernel(tiles, which_ref, wide_ref, keep, out_ref, state, mid):
    wide = wide_ref.shape[2]
    pad = BLOCK
    total = wide // BLOCK
    size = STEPS * time_step
    clear(mid, 5, tiles, (0, pad + wide))

    def put(block, i, olds, news):
        for f in range(3):
            out_ref[f, i, pl.ds(BLOCK * block, BLOCK), :] = news[f]

    linked = which_ref[0] > 2

    @pl.when(linked)
    def _():
        widen(state, wide_ref, wide, tiles, pad)
        first_stage(state, mid, keep, range(total), pad, size, tiles)
        second_stage(state, mid, keep, range(total), pad, size, tiles, put)

    @pl.when(jnp.logical_not(linked))
    def _():
        copy_rows(out_ref, lambda f, i, row, take: wide_ref[f, i, pl.ds(row, take), :], tiles, wide, 0, 0)


def first_link(which, wide, keep):
    tiles, rows = wide.shape[1:3]
    padded = (5, tiles, rows + 2 * BLOCK, LANES)
    return call(
        lambda *refs: link_kernel(tiles, *refs),
        "first_link",
        1,
        (array(*wide.shape),),
        [which, wide, keep],
        [scratch(*padded), scratch(*padded)],
    )[0]


def last_kernel(layout, which_ref, start_ref, keep, far_ref, *refs):
    strip, margin, tiles, chain = layout
    more_refs = refs[:-4]
    c_ref, f_ref, state, mid = refs[-4:]
    wide = strip + 2 * margin
    pad = BLOCK
    which = which_ref[0]
    total = wide // BLOCK
    coarse_size = STEPS * time_step

    clear(mid, 5, tiles, (0, pad + wide))

    def put(block, i, olds, news):
        store(state, i, pad + BLOCK * block, news)

    def add(defect, start_from):
        for f in range(3):
            for i in range(tiles):
                for b in range(0, wide - 4, BLOCK):
                    take = min(BLOCK, wide - 4 - b)
                    at = pl.ds(pad + 2 + b, take)
                    state[f, i, at, :] = start_from(f, i, 2 + b, take) + defect(f, i, b, take)
        for i in range(tiles):
            for b in range(0, wide, BLOCK):
                at = pl.ds(pad + b, BLOCK)
                height = 2.0 + state[0, i, at, :]
                state[3, i, at, :] = height * state[1, i, at, :]
                state[4, i, at, :] = height * state[2, i, at, :]

    def of_start(f, i, row, take):
        return start_ref[f, i, pl.ds(row, take), :]

    def of_state(f, i, row, take):
        return state[f, i, pl.ds(pad + row, take), :]

    def of_rows(ref):
        return lambda f, i, row, take: ref[f, i, pl.ds(row, take), :]

    def link(turn):
        if turn:
            first_stage(state, mid, keep, range(total), pad, coarse_size, tiles)
            second_stage(state, mid, keep, range(total), pad, coarse_size, tiles, put)
        defect = of_rows(more_refs[0].at[turn]) if more_refs else of_rows(far_ref)
        add(defect, of_state if turn else of_start)

    for turn in range(chain):
        pl.when(which > turn + 2)(lambda turn=turn: link(turn))
    pl.when(which <= 2)(lambda: widen(state, start_ref, wide, tiles, pad))

    first = margin // BLOCK
    strip_blocks = range(first, first + strip // BLOCK)

    early = which < 2

    def put_to(ref, value_of):
        def put_one(block, i, olds, news):
            at = pl.ds((block - first) * BLOCK, BLOCK)
            for f in range(3):
                value = value_of(f, i, at, news[f])
                ready[f].append(0.5 * value if f == 0 else value)
                if len(ready[f]) == tiles:
                    for p, natural in enumerate(gathered(ready[f])):
                        ref[f, at, pl.ds(p * LANES, LANES)] = natural
                    ready[f].clear()

        ready = [[], [], []]
        return put_one

    def c_value(f, i, at, new):
        return new

    def f_value(f, i, at, new):
        return jnp.where(early, far_ref[f, i, at, :], new)

    around = range(first - 1, first + strip // BLOCK + 1)
    first_stage(state, mid, keep, around, pad, coarse_size, tiles)
    second_stage(state, mid, keep, strip_blocks, pad, coarse_size, tiles, put_to(c_ref, c_value))

    def steps(blocks, group):
        def one(turn, carry):
            first_stage(state, mid, keep, blocks, pad, time_step, tiles)
            second_stage(state, mid, keep, blocks, pad, time_step, tiles, put)
            return carry

        if group > 0:
            lax.fori_loop(0, group, one, 0)

    near = min(BLOCK // 2 - 1, STEPS - 2)
    steps(range(total), STEPS - 2 - near)
    steps(around, near)
    first_stage(state, mid, keep, around, pad, time_step, tiles)
    second_stage(state, mid, keep, strip_blocks, pad, time_step, tiles, put_to(f_ref, f_value))


def last_chain(which, start, keep, far, more, strip, margin):
    tiles = start.shape[1]
    chain = more[0].shape[0] if more else 1
    layout = (strip, margin, tiles, chain)
    padded = (5, tiles, start.shape[2] + 2 * BLOCK, LANES)
    return call(
        lambda *refs: last_kernel(layout, *refs),
        "last_chain",
        3,
        (array(3, strip, tiles * LANES), array(3, strip, tiles * LANES)),
        [which, start, keep, far, *more],
        [scratch(*padded), scratch(*padded)],
    )


def body(initial_state, c_guess, friction):
    slices, strips = lax.axis_size("tm"), lax.axis_size("space")
    strip = initial_state.shape[1]
    which = lax.axis_index("tm")
    margin = 2 * (STEPS - 1) + 2 * (slices - 3)
    count = -(-(4 * STEPS + margin) // strip)
    both = ("tm", "space")

    def moved(value, target):
        pairs = []
        for t in range(slices):
            for s in range(strips):
                to = target(t, s)
                if to is not None:
                    pairs.append((t * strips + s, to[0] * strips + to[1] % strips))
        return lax.ppermute(value, both, pairs)

    place = lax.axis_index("space")
    paired = count == 2 and strips % 4 == 0
    side, turn = place % 2, place // 2 % 2
    spots = [4 - 4 * turn, 1 + 2 * side, jnp.full_like(side, 2), 3 - 2 * side, 4 * turn]
    index = jnp.stack([which, *spots]).astype(jnp.int32)
    start = jnp.where(which >= slices - 2, initial_state, c_guess[0])
    own = jnp.concatenate([start, friction[None]], axis=0)
    if paired:
        partner = moved(own, lambda t, s: (t, s ^ 1))
        one = moved(own, lambda t, s: (t, s ^ 2))
        other = moved(own, lambda t, s: (t, s - 2 if s // 2 % 2 == 0 else s + 2))
        relayed = moved(jnp.where(side == turn, one, other), lambda t, s: (t, s ^ 1))
        own, partner = deal(index, own, partner)
        one, other = deal(index, one, other)
        parts = [one, relayed, own, partner, other]
    else:
        parts = []
        for offset in range(-count, count + 1):
            parts.append(own if offset == 0 else moved(own, lambda t, s, o=offset: (t, s - o)))
        parts = list(deal(index, *parts))
    narrow, far, wide, keep = fine_chain(index, parts, margin, slices, paired)

    got_far = moved(far, lambda t, s: (slices - 1 - t, s))
    got = moved(narrow, lambda t, s: ((t + 2) % slices, s))
    more = []
    if slices != 4:
        everyone = lax.all_gather(wide, "tm", axis=0)
        more = [everyone[: slices - 3, :, :, 2:-2]]
        wide = everyone[slices - 1]
    first = first_link(index, wide, keep)
    coarse, f_points = last_chain(index, first, keep, got_far, more, strip, margin)
    c_points = jnp.where(which < 2, got, coarse + got)
    return (c_points[None], f_points[None])


def solution(mesh):
    placed = (P(None, "space", None), P("tm", None, "space", None), P("space", None))
    return jax.shard_map(
        body,
        mesh=mesh,
        in_specs=placed,
        out_specs=(P("tm", None, "space", None), P("tm", None, "space", None)),
        check_vma=False,
    )
```

```python
import jax
import jax.numpy as jnp
from jax import lax
from jax.experimental import pallas as pl
from jax.experimental.pallas import tpu as pltpu
from jax.sharding import PartitionSpec as P

STEPS = 8


gravity = 2.0
coriolis = 0.5
viscosity = 0.5
time_step = 0.04

LANES = 128
BLOCK = 8
VMEM = pl.BlockSpec(memory_space=pltpu.VMEM)
VMEM_LIMIT = 8 * 2**20
FLOPS_PER_US = 500_000_000


def lanes():
    return lax.broadcasted_iota(jnp.int32, (BLOCK, LANES), 1)


def pick(tile, index):
    return jnp.take_along_axis(tile, index, axis=1, mode="promise_in_bounds")


def dealt(natural):
    tiles = len(natural)
    out = []
    for i in range(tiles):
        column = tiles * lanes() + i
        index = lax.rem(column, LANES)
        value = pick(natural[0], index)
        for p in range(1, tiles):
            value = jnp.where(column >= p * LANES, pick(natural[p], index), value)
        out.append(value)
    return out


def gathered(tiled):
    tiles = len(tiled)
    out = []
    for p in range(tiles):
        column = p * LANES + lanes()
        index = column // tiles
        which = lax.rem(column, tiles)
        value = pick(tiled[0], index)
        for i in range(1, tiles):
            value = jnp.where(which == i, pick(tiled[i], index), value)
        out.append(value)
    return out


def east(tiled):
    return tiled[1:] + [pltpu.roll(tiled[0], LANES - 1, 1)]


def west(tiled):
    return [pltpu.roll(tiled[-1], 1, 1)] + tiled[:-1]


def slopes(src, row, tiles):
    def rows(plane, by):
        return [src[plane, i, pl.ds(row + by, BLOCK), :] for i in range(tiles)]

    here = [rows(f, 0) for f in range(3)]
    north = [rows(f, 1) for f in range(4)]
    south = [rows(f, -1) for f in range(4)]
    flux = rows(4, 0)
    easts = [east(value) for value in here + [flux]]
    wests = [west(value) for value in here + [flux]]
    out = []
    for i in range(tiles):
        u, w = here[1][i], here[2][i]
        en, un, wn, fn = (north[f][i] for f in range(4))
        es, us, ws, fs = (south[f][i] for f in range(4))
        ee, ue, we, ge = (easts[f][i] for f in range(4))
        ew, uw, ww, gw = (wests[f][i] for f in range(4))
        rest_e = ((en + es) + (ee + ew)) - ((fn - fs) + (ge - gw))
        rest_u = ((un + us) - u * (un - us)) + ((ue + uw) - w * (ue - uw))
        rest_w = ((wn + ws) - u * (wn - ws)) + ((we + ww) - w * (we - ww))
        rest_u = rest_u + (w - (en - es))
        rest_w = rest_w - (u + (ee - ew))
        out.append((rest_e, rest_u, rest_w))
    return here, out


def own_factor(keep, i, row, size):
    kept = keep[i, pl.ds(row, BLOCK), :]
    ratio = size / time_step
    return kept if ratio == 1.0 else ratio * kept + (1.0 - ratio)


def store(ref, i, row, value):
    at = pl.ds(row, BLOCK)
    for f in range(3):
        ref[f, i, at, :] = value[f]
    height = 2.0 + value[0]
    ref[3, i, at, :] = height * value[1]
    ref[4, i, at, :] = height * value[2]


def first_stage(src, mid, keep, blocks, pad, size, tiles):
    for block in blocks:
        row = pad + BLOCK * block
        here, rest = slopes(src, row, tiles)
        for i in range(tiles):
            factor = own_factor(keep, i, row, size)
            value = []
            for f in range(3):
                own = (1.0 - 2.0 * size) if f == 0 else factor
                value.append(own * here[f][i] + (0.5 * size) * rest[i][f])
            store(mid, i, row, value)


def second_stage(src, mid, keep, blocks, pad, size, tiles, put):
    for block in blocks:
        row = pad + BLOCK * block
        here, rest = slopes(mid, row, tiles)
        for i in range(tiles):
            factor = own_factor(keep, i, row, size)
            olds, news = [], []
            for f in range(3):
                own = (1.0 - 2.0 * size) if f == 0 else factor
                old = src[f, i, pl.ds(row, BLOCK), :]
                olds.append(old)
                news.append(0.5 * ((old + own * here[f][i]) + (0.5 * size) * rest[i][f]))
            put(block, i, olds, news)


def clear(ref, planes, tiles, starts):
    for f in range(planes):
        for i in range(tiles):
            for row in starts:
                ref[f, i, pl.ds(row, BLOCK), :] = jnp.zeros((BLOCK, LANES), jnp.float32)


def copy_rows(target, source, tiles, row_count, to, start):
    for f in range(3):
        for i in range(tiles):
            for b in range(0, row_count, BLOCK):
                take = min(BLOCK, row_count - b)
                target[f, i, pl.ds(to + b, take), :] = source(f, i, start + b, take)


def copy_natural(target, source, tiles, row_count, start):
    for f in range(3):
        for b in range(0, row_count, BLOCK):
            tiled = [source(f, i, start + b, BLOCK) for i in range(tiles)]
            for p, value in enumerate(gathered(tiled)):
                target[f, pl.ds(b, BLOCK), pl.ds(p * LANES, LANES)] = 0.5 * value if f == 0 else value


def fine_kernel(layout, standing_at, *refs):
    count, strip, margin, tiles, slices, paired = layout
    parts = refs[: 2 * count + 1]
    far_ref, raw_ref, start_ref, relaxed_ref, coarse, factor_ref, state, mid, keep, before = refs[2 * count + 1 :]
    rows = (2 * count + 1) * strip
    pad = BLOCK
    centre = count * strip // BLOCK
    strip_blocks = range(centre, centre + strip // BLOCK)
    total = rows // BLOCK
    which = standing_at[0]

    for ref in (state, mid):
        clear(ref, 5, tiles, (0, pad + rows))

    def load(p, part):
        for b in range(0, strip, BLOCK):
            row = pad + p * strip + b
            if not isinstance(p, int):
                row = pl.multiple_of(row, BLOCK)
            if len(part.shape) == 4:
                planes = [[part[f, i, pl.ds(b, BLOCK), :] for i in range(tiles)] for f in range(4)]
            else:
                planes = dealt_block(part, b, tiles)
            for i in range(tiles):
                store(state, i, row, [planes[f][i] for f in range(3)])
                keep[i, pl.ds(row, BLOCK), :] = planes[3][i]

    for p, part in enumerate(parts):
        load(standing_at[1 + p] if paired and p != count else p, part)

    def put(block, i, olds, news):
        if block in strip_blocks:
            for f in range(3):
                before[f, i, pl.ds((block - centre) * BLOCK, BLOCK), :] = olds[f]
        store(state, i, pad + BLOCK * block, news)

    def steps(start, group):
        first, last = start // BLOCK, total - start // BLOCK

        def one(turn, carry):
            first_stage(state, mid, keep, range(first, last), pad, time_step, tiles)
            second_stage(state, mid, keep, range(first, last), pad, time_step, tiles, put)
            return carry

        lax.fori_loop(0, group, one, 0)

    def from_state(f, i, row, take):
        return state[f, i, pl.ds(pad + row, take), :]

    def from_before(f, i, row, take):
        return before[f, i, pl.ds(row, take), :]

    wide = strip + 2 * margin
    edge = count * strip - margin
    out_first, out_last = edge // BLOCK, (edge + wide) // BLOCK
    window = wide + 2 * BLOCK
    for i in range(tiles):
        for b in range(0, window + 2 * pad, BLOCK):
            factor_ref[i, pl.ds(b, BLOCK), :] = keep[i, pl.ds(edge - BLOCK + b, BLOCK), :]
    copy_rows(start_ref, from_state, tiles, window, 0, edge - BLOCK)

    group = BLOCK // 2
    for start in range(0, STEPS, group):
        steps(2 * start, group)
    copy_rows(relaxed_ref, from_state, tiles, window, 0, edge - BLOCK)

    @pl.when(which == slices - 1)
    def _():
        copy_rows(far_ref, from_before, tiles, strip, 0, 0)

    def put_coarse(block, i, olds, news):
        for f in range(3):
            coarse[f, i, pl.ds((block - out_first) * BLOCK, BLOCK), :] = news[f]

    size = STEPS * time_step
    first_stage(state, mid, keep, range(out_first - 1, out_last + 1), pad, size, tiles)
    second_stage(state, mid, keep, range(out_first, out_last), pad, size, tiles, put_coarse)

    for start in range(STEPS, 2 * STEPS, group):
        steps(2 * start, group)

    def from_defect(f, i, row, take):
        return state[f, i, pl.ds(pad + row, take), :] - coarse[f, i, pl.ds(row - edge, take), :]

    @pl.when(which < slices - 2)
    def _():
        copy_rows(far_ref, from_defect, tiles, wide - 4, 0, edge + 2)
        copy_rows(raw_ref, from_defect, tiles, wide, 0, edge)

    @pl.when(which >= slices - 2)
    def _():
        copy_rows(raw_ref, from_state, tiles, wide, 0, edge)

    @pl.when(which == slices - 2)
    def _():
        copy_rows(far_ref, from_before, tiles, strip, 0, 0)


def array(*shape):
    return jax.ShapeDtypeStruct(shape, jnp.float32)


def scratch(*shape):
    return pltpu.VMEM(shape, jnp.float32)


def standing():
    place = lax.axis_index("space")
    side, turn = lax.rem(place, 2), lax.rem(lax.div(place, 2), 2)
    return [lax.axis_index("tm"), 4 - 4 * turn, 1 + 2 * side, 2, 3 - 2 * side, 4 * turn]


def call(kernel, name, micros, out_shape, args, scratches=()):
    return pl.pallas_call(
        lambda *refs: kernel(standing(), *refs),
        name=name,
        out_shape=out_shape,
        in_specs=[VMEM] * len(args),
        out_specs=tuple(VMEM for _ in out_shape),
        scratch_shapes=list(scratches),
        compiler_params=pltpu.CompilerParams(vmem_limit_bytes=VMEM_LIMIT),
        cost_estimate=pl.CostEstimate(flops=int(micros * FLOPS_PER_US), bytes_accessed=0, transcendentals=0),
    )(*args)


def dealt_block(ref, b, tiles):
    out = []
    for f in range(4):
        tiled = dealt([ref[f, pl.ds(b, BLOCK), pl.ds(p * LANES, LANES)] for p in range(tiles)])
        if f == 0:
            tiled = [2.0 * value for value in tiled]
        if f == 3:
            tiled = [(1.0 - 2.0 * time_step) - time_step * value for value in tiled]
        out.append(tiled)
    return out


def deal_kernel(tiles, standing_at, *refs):
    half = len(refs) // 2
    for ref, out_ref in zip(refs[:half], refs[half:]):
        for b in range(0, ref.shape[1], BLOCK):
            for f, tiled in enumerate(dealt_block(ref, b, tiles)):
                for i, value in enumerate(tiled):
                    out_ref[f, i, pl.ds(b, BLOCK), :] = value


def deal(*parts):
    strip, columns = parts[0].shape[1:]
    tiles = columns // LANES
    out = tuple(array(4, tiles, strip, LANES) for _ in parts)
    return call(lambda *refs: deal_kernel(tiles, *refs), "deal", 0.5, out, list(parts))


def fine_chain(parts, margin, slices, paired):
    count = len(parts) // 2
    tiles, strip = parts[0].shape[1:3]
    wide = strip + 2 * margin
    rows = len(parts) * strip + 2 * BLOCK
    layout = (count, strip, margin, tiles, slices, paired)
    return call(
        lambda *refs: fine_kernel(layout, *refs),
        "fine_chain",
        8,
        (
            array(3, tiles, wide - 4, LANES),
            array(3, tiles, wide, LANES),
            array(3, tiles, wide + 2 * BLOCK, LANES),
            array(3, tiles, wide + 2 * BLOCK, LANES),
            array(3, tiles, wide, LANES),
            array(tiles, wide + 4 * BLOCK, LANES),
        ),
        list(parts),
        [
            scratch(5, tiles, rows, LANES),
            scratch(5, tiles, rows, LANES),
            scratch(tiles, rows, LANES),
            scratch(3, tiles, strip, LANES),
        ],
    )


def widen(state, wide_ref, wide, tiles, pad):
    clear(state, 5, tiles, (0, pad + wide))
    for i in range(tiles):
        for b in range(0, wide, BLOCK):
            store(state, i, pad + b, [wide_ref[f, i, pl.ds(b, BLOCK), :] for f in range(3)])


def settle_kernel(layout, standing_at, raw_ref, start_ref, relaxed_ref, coarse_ref, keep, *refs):
    narrow_ref, wide_ref, state, mid = refs
    strip, margin, tiles, slices = layout
    wide = strip + 2 * margin
    window = wide + 2 * BLOCK
    pad = BLOCK
    total = window // BLOCK
    which = standing_at[0]
    size = STEPS * time_step

    def rows_of(ref, lift=0):
        return lambda f, i, row, take: ref[f, i, pl.ds(lift + row, take), :]

    def put_first(block, i, olds, news):
        at = pl.ds(BLOCK * block, BLOCK)
        first = [news[f] + (relaxed_ref[f, i, at, :] - news[f]) for f in range(3)]
        store(state, i, pad + BLOCK * block, first)

    def put_second(block, i, olds, news):
        at = pl.ds(BLOCK * (block - 1), BLOCK)
        for f in range(3):
            wide_ref[f, i, at, :] = news[f] + (raw_ref[f, i, at, :] - coarse_ref[f, i, at, :])

    @pl.when(which < slices - 2)
    def _():
        copy_rows(wide_ref, rows_of(raw_ref), tiles, wide, 0, 0)
        copy_natural(narrow_ref, rows_of(raw_ref), tiles, strip, margin)

    @pl.when(which >= slices - 2)
    def _():
        clear(mid, 5, tiles, (0, pad + window))
        widen(state, start_ref, window, tiles, pad)
        first_stage(state, mid, keep, range(total), pad, size, tiles)
        second_stage(state, mid, keep, range(total), pad, size, tiles, put_first)

        @pl.when(which == slices - 2)
        def _():
            copy_natural(narrow_ref, rows_of(state, pad), tiles, strip, BLOCK + margin)

        first_stage(state, mid, keep, range(total), pad, size, tiles)
        second_stage(state, mid, keep, range(1, total - 1), pad, size, tiles, put_second)

        @pl.when(which == slices - 1)
        def _():
            copy_natural(narrow_ref, rows_of(wide_ref), tiles, strip, margin)


def settle(raw, start, relaxed, coarse, keep, strip, margin, slices):
    tiles, wide = raw.shape[1:3]
    layout = (strip, margin, tiles, slices)
    padded = (5, tiles, wide + 4 * BLOCK, LANES)
    return call(
        lambda *refs: settle_kernel(layout, *refs),
        "settle",
        1,
        (array(3, strip, tiles * LANES), array(3, tiles, wide, LANES)),
        [raw, start, relaxed, coarse, keep],
        [scratch(*padded), scratch(*padded)],
    )


def inner(keep):
    return keep.at[:, pl.ds(BLOCK, keep.shape[1] - 2 * BLOCK), :]


def link_kernel(tiles, standing_at, wide_ref, keep, out_ref, state, mid):
    wide = wide_ref.shape[2]
    pad = BLOCK
    total = wide // BLOCK
    size = STEPS * time_step
    keep = inner(keep)
    clear(mid, 5, tiles, (0, pad + wide))

    def put(block, i, olds, news):
        for f in range(3):
            out_ref[f, i, pl.ds(BLOCK * block, BLOCK), :] = news[f]

    linked = standing_at[0] > 2

    @pl.when(linked)
    def _():
        widen(state, wide_ref, wide, tiles, pad)
        first_stage(state, mid, keep, range(total), pad, size, tiles)
        second_stage(state, mid, keep, range(total), pad, size, tiles, put)

    @pl.when(jnp.logical_not(linked))
    def _():
        copy_rows(out_ref, lambda f, i, row, take: wide_ref[f, i, pl.ds(row, take), :], tiles, wide, 0, 0)


def first_link(wide, keep):
    tiles, rows = wide.shape[1:3]
    padded = (5, tiles, rows + 2 * BLOCK, LANES)
    return call(
        lambda *refs: link_kernel(tiles, *refs),
        "first_link",
        1,
        (array(*wide.shape),),
        [wide, keep],
        [scratch(*padded), scratch(*padded)],
    )[0]


def last_kernel(layout, standing_at, start_ref, keep, far_ref, *refs):
    strip, margin, tiles, chain = layout
    more_refs = refs[:-4]
    c_ref, f_ref, state, mid = refs[-4:]
    wide = strip + 2 * margin
    pad = BLOCK
    which = standing_at[0]
    total = wide // BLOCK
    coarse_size = STEPS * time_step
    keep = inner(keep)

    clear(mid, 5, tiles, (0, pad + wide))

    def put(block, i, olds, news):
        store(state, i, pad + BLOCK * block, news)

    def add(defect, start_from):
        for f in range(3):
            for i in range(tiles):
                for b in range(0, wide - 4, BLOCK):
                    take = min(BLOCK, wide - 4 - b)
                    at = pl.ds(pad + 2 + b, take)
                    state[f, i, at, :] = start_from(f, i, 2 + b, take) + defect(f, i, b, take)
        for i in range(tiles):
            for b in range(0, wide, BLOCK):
                at = pl.ds(pad + b, BLOCK)
                height = 2.0 + state[0, i, at, :]
                state[3, i, at, :] = height * state[1, i, at, :]
                state[4, i, at, :] = height * state[2, i, at, :]

    def of_start(f, i, row, take):
        return start_ref[f, i, pl.ds(row, take), :]

    def of_state(f, i, row, take):
        return state[f, i, pl.ds(pad + row, take), :]

    def of_rows(ref):
        return lambda f, i, row, take: ref[f, i, pl.ds(row, take), :]

    def link(turn):
        if turn:
            first_stage(state, mid, keep, range(total), pad, coarse_size, tiles)
            second_stage(state, mid, keep, range(total), pad, coarse_size, tiles, put)
        defect = of_rows(more_refs[0].at[turn]) if more_refs else of_rows(far_ref)
        add(defect, of_state if turn else of_start)

    for turn in range(chain):
        pl.when(which > turn + 2)(lambda turn=turn: link(turn))
    pl.when(which <= 2)(lambda: widen(state, start_ref, wide, tiles, pad))

    first = margin // BLOCK
    strip_blocks = range(first, first + strip // BLOCK)

    early = which < 2

    def put_to(ref, value_of):
        def put_one(block, i, olds, news):
            at = pl.ds((block - first) * BLOCK, BLOCK)
            for f in range(3):
                value = value_of(f, i, at, news[f])
                ready[f].append(0.5 * value if f == 0 else value)
                if len(ready[f]) == tiles:
                    for p, natural in enumerate(gathered(ready[f])):
                        ref[f, at, pl.ds(p * LANES, LANES)] = natural
                    ready[f].clear()

        ready = [[], [], []]
        return put_one

    def c_value(f, i, at, new):
        return new

    def f_value(f, i, at, new):
        return jnp.where(early, far_ref[f, i, at, :], new)

    around = range(first - 1, first + strip // BLOCK + 1)
    first_stage(state, mid, keep, around, pad, coarse_size, tiles)
    second_stage(state, mid, keep, strip_blocks, pad, coarse_size, tiles, put_to(c_ref, c_value))

    def steps(blocks, group):
        def one(turn, carry):
            first_stage(state, mid, keep, blocks, pad, time_step, tiles)
            second_stage(state, mid, keep, blocks, pad, time_step, tiles, put)
            return carry

        if group > 0:
            lax.fori_loop(0, group, one, 0)

    near = min(BLOCK // 2 - 1, STEPS - 2)
    steps(range(total), STEPS - 2 - near)
    steps(around, near)
    first_stage(state, mid, keep, around, pad, time_step, tiles)
    second_stage(state, mid, keep, strip_blocks, pad, time_step, tiles, put_to(f_ref, f_value))


def last_chain(start, keep, far, more, strip, margin):
    tiles = start.shape[1]
    chain = more[0].shape[0] if more else 1
    layout = (strip, margin, tiles, chain)
    padded = (5, tiles, start.shape[2] + 2 * BLOCK, LANES)
    return call(
        lambda *refs: last_kernel(layout, *refs),
        "last_chain",
        3,
        (array(3, strip, tiles * LANES), array(3, strip, tiles * LANES)),
        [start, keep, far, *more],
        [scratch(*padded), scratch(*padded)],
    )


def body(initial_state, c_guess, friction):
    slices, strips = lax.axis_size("tm"), lax.axis_size("space")
    strip = initial_state.shape[1]
    which = lax.axis_index("tm")
    margin = 2 * (STEPS - 1) + 2 * (slices - 3)
    count = -(-(4 * STEPS + margin) // strip)
    both = ("tm", "space")

    def moved(value, target):
        pairs = []
        for t in range(slices):
            for s in range(strips):
                to = target(t, s)
                if to is not None:
                    pairs.append((t * strips + s, to[0] * strips + to[1] % strips))
        return lax.ppermute(value, both, pairs)

    place = lax.axis_index("space")
    paired = count == 2 and strips % 4 == 0
    side, turn = place % 2, place // 2 % 2
    start = jnp.where(which >= slices - 2, initial_state, c_guess[0])
    own = jnp.concatenate([start, friction[None]], axis=0)
    if paired:
        partner = moved(own, lambda t, s: (t, s ^ 1))
        one = moved(own, lambda t, s: (t, s ^ 2))
        other = moved(own, lambda t, s: (t, s - 2 if s // 2 % 2 == 0 else s + 2))
        relayed = moved(jnp.where(side == turn, one, other), lambda t, s: (t, s ^ 1))
        own, partner, one, other = deal(own, partner, one, other)
        parts = [one, relayed, own, partner, other]
    else:
        parts = []
        for offset in range(-count, count + 1):
            parts.append(own if offset == 0 else moved(own, lambda t, s, o=offset: (t, s - o)))
        parts = list(deal(*parts))
    far, raw, begin, relaxed, stepped, keep = fine_chain(parts, margin, slices, paired)

    got_far = moved(far, lambda t, s: (slices - 1 - t, s))
    narrow, wide = settle(raw, begin, relaxed, stepped, keep, strip, margin, slices)
    got = moved(narrow, lambda t, s: ((t + 2) % slices, s))
    more = []
    if slices != 4:
        everyone = lax.all_gather(wide, "tm", axis=0)
        more = [everyone[: slices - 3, :, :, 2:-2]]
        wide = everyone[slices - 1]
    first = first_link(wide, keep)
    coarse, f_points = last_chain(first, keep, got_far, more, strip, margin)
    c_points = jnp.where(which < 2, got, coarse + got)
    return (c_points[None], f_points[None])


def solution(mesh):
    placed = (P(None, "space", None), P("tm", None, "space", None), P("space", None))
    return jax.shard_map(
        body,
        mesh=mesh,
        in_specs=placed,
        out_specs=(P("tm", None, "space", None), P("tm", None, "space", None)),
        check_vma=False,
    )
```

```python
import jax
import jax.numpy as jnp
from jax import lax
from jax.experimental import pallas as pl
from jax.experimental.pallas import tpu as pltpu
from jax.sharding import PartitionSpec as P

STEPS = 8


gravity = 2.0
coriolis = 0.5
viscosity = 0.5
time_step = 0.04

LANES = 128
BLOCK = 8
VMEM = pl.BlockSpec(memory_space=pltpu.VMEM)
VMEM_LIMIT = 8 * 2**20
FLOPS_PER_US = 500_000_000


def lanes():
    return lax.broadcasted_iota(jnp.int32, (BLOCK, LANES), 1)


def pick(tile, index):
    return jnp.take_along_axis(tile, index, axis=1, mode="promise_in_bounds")


def dealt(natural):
    tiles = len(natural)
    out = []
    for i in range(tiles):
        column = tiles * lanes() + i
        index = lax.rem(column, LANES)
        value = pick(natural[0], index)
        for p in range(1, tiles):
            value = jnp.where(column >= p * LANES, pick(natural[p], index), value)
        out.append(value)
    return out


def gathered(tiled):
    tiles = len(tiled)
    out = []
    for p in range(tiles):
        column = p * LANES + lanes()
        index = column // tiles
        which = lax.rem(column, tiles)
        value = pick(tiled[0], index)
        for i in range(1, tiles):
            value = jnp.where(which == i, pick(tiled[i], index), value)
        out.append(value)
    return out


def east(tiled):
    return tiled[1:] + [pltpu.roll(tiled[0], LANES - 1, 1)]


def west(tiled):
    return [pltpu.roll(tiled[-1], 1, 1)] + tiled[:-1]


def slopes(src, row, tiles):
    def rows(plane, by):
        return [src[plane, i, pl.ds(row + by, BLOCK), :] for i in range(tiles)]

    here = [rows(f, 0) for f in range(3)]
    north = [rows(f, 1) for f in range(4)]
    south = [rows(f, -1) for f in range(4)]
    flux = rows(4, 0)
    easts = [east(value) for value in here + [flux]]
    wests = [west(value) for value in here + [flux]]
    out = []
    for i in range(tiles):
        u, w = here[1][i], here[2][i]
        en, un, wn, fn = (north[f][i] for f in range(4))
        es, us, ws, fs = (south[f][i] for f in range(4))
        ee, ue, we, ge = (easts[f][i] for f in range(4))
        ew, uw, ww, gw = (wests[f][i] for f in range(4))
        rest_e = ((en + es) + (ee + ew)) - ((fn - fs) + (ge - gw))
        rest_u = ((un + us) - u * (un - us)) + ((ue + uw) - w * (ue - uw))
        rest_w = ((wn + ws) - u * (wn - ws)) + ((we + ww) - w * (we - ww))
        rest_u = rest_u + (w - (en - es))
        rest_w = rest_w - (u + (ee - ew))
        out.append((rest_e, rest_u, rest_w))
    return here, out


def own_factor(keep, i, row, size):
    kept = keep[i, pl.ds(row, BLOCK), :]
    ratio = size / time_step
    return kept if ratio == 1.0 else ratio * kept + (1.0 - ratio)


def store(ref, i, row, value):
    at = pl.ds(row, BLOCK)
    for f in range(3):
        ref[f, i, at, :] = value[f]
    height = 2.0 + value[0]
    ref[3, i, at, :] = height * value[1]
    ref[4, i, at, :] = height * value[2]


def first_stage(src, mid, keep, blocks, pad, size, tiles):
    for block in blocks:
        row = pad + BLOCK * block
        here, rest = slopes(src, row, tiles)
        for i in range(tiles):
            factor = own_factor(keep, i, row, size)
            value = []
            for f in range(3):
                own = (1.0 - 2.0 * size) if f == 0 else factor
                value.append(own * here[f][i] + (0.5 * size) * rest[i][f])
            store(mid, i, row, value)


def second_stage(src, mid, keep, blocks, pad, size, tiles, put):
    for block in blocks:
        row = pad + BLOCK * block
        here, rest = slopes(mid, row, tiles)
        for i in range(tiles):
            factor = own_factor(keep, i, row, size)
            olds, news = [], []
            for f in range(3):
                own = (1.0 - 2.0 * size) if f == 0 else factor
                old = src[f, i, pl.ds(row, BLOCK), :]
                olds.append(old)
                news.append(0.5 * ((old + own * here[f][i]) + (0.5 * size) * rest[i][f]))
            put(block, i, olds, news)


def clear(ref, planes, tiles, starts):
    for f in range(planes):
        for i in range(tiles):
            for row in starts:
                ref[f, i, pl.ds(row, BLOCK), :] = jnp.zeros((BLOCK, LANES), jnp.float32)


def copy_rows(target, source, tiles, row_count, to, start):
    for f in range(3):
        for i in range(tiles):
            for b in range(0, row_count, BLOCK):
                take = min(BLOCK, row_count - b)
                target[f, i, pl.ds(to + b, take), :] = source(f, i, start + b, take)


def copy_natural(target, source, tiles, row_count, start):
    for f in range(3):
        for b in range(0, row_count, BLOCK):
            tiled = [source(f, i, start + b, BLOCK) for i in range(tiles)]
            for p, value in enumerate(gathered(tiled)):
                target[f, pl.ds(b, BLOCK), pl.ds(p * LANES, LANES)] = 0.5 * value if f == 0 else value


def fine_kernel(layout, standing_at, *refs):
    count, strip, margin, tiles, slices, paired = layout
    parts = refs[: 2 * count + 1]
    far_ref, raw_ref, start_ref, relaxed_ref, coarse, factor_ref, state, mid, keep, before = refs[2 * count + 1 :]
    rows = (2 * count + 1) * strip
    pad = BLOCK
    centre = count * strip // BLOCK
    strip_blocks = range(centre, centre + strip // BLOCK)
    total = rows // BLOCK
    which = standing_at[0]

    for ref in (state, mid):
        clear(ref, 5, tiles, (0, pad + rows))

    def load(p, part):
        for b in range(0, strip, BLOCK):
            row = pad + p * strip + b
            if not isinstance(p, int):
                row = pl.multiple_of(row, BLOCK)
            if len(part.shape) == 4:
                planes = [[part[f, i, pl.ds(b, BLOCK), :] for i in range(tiles)] for f in range(4)]
            else:
                planes = dealt_block(part, b, tiles)
            for i in range(tiles):
                store(state, i, row, [planes[f][i] for f in range(3)])
                keep[i, pl.ds(row, BLOCK), :] = planes[3][i]

    for p, part in enumerate(parts):
        load(standing_at[1 + p] if paired and p != count else p, part)

    def put(block, i, olds, news):
        if block in strip_blocks:
            for f in range(3):
                before[f, i, pl.ds((block - centre) * BLOCK, BLOCK), :] = olds[f]
        store(state, i, pad + BLOCK * block, news)

    def steps(start, group):
        first, last = start // BLOCK, total - start // BLOCK

        def one(turn, carry):
            first_stage(state, mid, keep, range(first, last), pad, time_step, tiles)
            second_stage(state, mid, keep, range(first, last), pad, time_step, tiles, put)
            return carry

        lax.fori_loop(0, group, one, 0)

    def from_state(f, i, row, take):
        return state[f, i, pl.ds(pad + row, take), :]

    def from_before(f, i, row, take):
        return before[f, i, pl.ds(row, take), :]

    wide = strip + 2 * margin
    edge = count * strip - margin
    out_first, out_last = edge // BLOCK, (edge + wide) // BLOCK
    window = wide + 2 * BLOCK
    for i in range(tiles):
        for b in range(0, window + 2 * pad, BLOCK):
            factor_ref[i, pl.ds(b, BLOCK), :] = keep[i, pl.ds(edge - BLOCK + b, BLOCK), :]
    copy_rows(start_ref, from_state, tiles, window, 0, edge - BLOCK)

    group = BLOCK // 2
    for start in range(0, STEPS, group):
        steps(2 * start, group)
    copy_rows(relaxed_ref, from_state, tiles, window, 0, edge - BLOCK)

    @pl.when(which == slices - 1)
    def _():
        copy_rows(far_ref, from_before, tiles, strip, 0, 0)

    def put_coarse(block, i, olds, news):
        for f in range(3):
            coarse[f, i, pl.ds((block - out_first) * BLOCK, BLOCK), :] = news[f]

    size = STEPS * time_step
    first_stage(state, mid, keep, range(out_first - 1, out_last + 1), pad, size, tiles)
    second_stage(state, mid, keep, range(out_first, out_last), pad, size, tiles, put_coarse)

    for start in range(STEPS, 2 * STEPS, group):
        steps(2 * start, group)

    def from_defect(f, i, row, take):
        return state[f, i, pl.ds(pad + row, take), :] - coarse[f, i, pl.ds(row - edge, take), :]

    @pl.when(which < slices - 2)
    def _():
        copy_rows(far_ref, from_defect, tiles, wide - 4, 0, edge + 2)
        copy_rows(raw_ref, from_defect, tiles, wide, 0, edge)

    @pl.when(which >= slices - 2)
    def _():
        copy_rows(raw_ref, from_state, tiles, wide, 0, edge)

    @pl.when(which == slices - 2)
    def _():
        copy_rows(far_ref, from_before, tiles, strip, 0, 0)


def array(*shape):
    return jax.ShapeDtypeStruct(shape, jnp.float32)


def scratch(*shape):
    return pltpu.VMEM(shape, jnp.float32)


def standing():
    place = lax.axis_index("space")
    side, turn = lax.rem(place, 2), lax.rem(lax.div(place, 2), 2)
    return [lax.axis_index("tm"), 4 - 4 * turn, 1 + 2 * side, 2, 3 - 2 * side, 4 * turn]


def call(kernel, name, micros, out_shape, args, scratches=()):
    return pl.pallas_call(
        lambda *refs: kernel(standing(), *refs),
        name=name,
        out_shape=out_shape,
        in_specs=[VMEM] * len(args),
        out_specs=tuple(VMEM for _ in out_shape),
        scratch_shapes=list(scratches),
        compiler_params=pltpu.CompilerParams(vmem_limit_bytes=VMEM_LIMIT),
        cost_estimate=pl.CostEstimate(flops=int(micros * FLOPS_PER_US), bytes_accessed=0, transcendentals=0),
    )(*args)


def dealt_block(ref, b, tiles):
    out = []
    for f in range(4):
        tiled = dealt([ref[f, pl.ds(b, BLOCK), pl.ds(p * LANES, LANES)] for p in range(tiles)])
        if f == 0:
            tiled = [2.0 * value for value in tiled]
        if f == 3:
            tiled = [(1.0 - 2.0 * time_step) - time_step * value for value in tiled]
        out.append(tiled)
    return out


def deal_kernel(tiles, standing_at, *refs):
    half = len(refs) // 2
    for ref, out_ref in zip(refs[:half], refs[half:]):
        for b in range(0, ref.shape[1], BLOCK):
            for f, tiled in enumerate(dealt_block(ref, b, tiles)):
                for i, value in enumerate(tiled):
                    out_ref[f, i, pl.ds(b, BLOCK), :] = value


def deal(*parts):
    strip, columns = parts[0].shape[1:]
    tiles = columns // LANES
    out = tuple(array(4, tiles, strip, LANES) for _ in parts)
    return call(lambda *refs: deal_kernel(tiles, *refs), "deal", 0.5, out, list(parts))


def fine_chain(parts, margin, slices, paired):
    count = len(parts) // 2
    tiles, strip = parts[0].shape[1:3]
    wide = strip + 2 * margin
    rows = len(parts) * strip + 2 * BLOCK
    layout = (count, strip, margin, tiles, slices, paired)
    return call(
        lambda *refs: fine_kernel(layout, *refs),
        "fine_chain",
        8,
        (
            array(3, tiles, wide - 4, LANES),
            array(3, tiles, wide, LANES),
            array(3, tiles, wide + 2 * BLOCK, LANES),
            array(3, tiles, wide + 2 * BLOCK, LANES),
            array(3, tiles, wide, LANES),
            array(tiles, wide + 4 * BLOCK, LANES),
        ),
        list(parts),
        [
            scratch(5, tiles, rows, LANES),
            scratch(5, tiles, rows, LANES),
            scratch(tiles, rows, LANES),
            scratch(3, tiles, strip, LANES),
        ],
    )


def widen(state, wide_ref, wide, tiles, pad):
    clear(state, 5, tiles, (0, pad + wide))
    for i in range(tiles):
        for b in range(0, wide, BLOCK):
            store(state, i, pad + b, [wide_ref[f, i, pl.ds(b, BLOCK), :] for f in range(3)])


def settle_kernel(layout, standing_at, raw_ref, start_ref, relaxed_ref, coarse_ref, keep, *refs):
    narrow_ref, wide_ref, state, mid = refs
    strip, margin, tiles, slices = layout
    wide = strip + 2 * margin
    window = wide + 2 * BLOCK
    pad = BLOCK
    total = window // BLOCK
    which = standing_at[0]
    size = STEPS * time_step

    def rows_of(ref, lift=0):
        return lambda f, i, row, take: ref[f, i, pl.ds(lift + row, take), :]

    def put_first(block, i, olds, news):
        at = pl.ds(BLOCK * block, BLOCK)
        first = [news[f] + (relaxed_ref[f, i, at, :] - news[f]) for f in range(3)]
        store(state, i, pad + BLOCK * block, first)

    def put_second(block, i, olds, news):
        at = pl.ds(BLOCK * (block - 1), BLOCK)
        for f in range(3):
            wide_ref[f, i, at, :] = news[f] + (raw_ref[f, i, at, :] - coarse_ref[f, i, at, :])

    @pl.when(which < slices - 2)
    def _():
        copy_rows(wide_ref, rows_of(raw_ref), tiles, wide, 0, 0)
        copy_natural(narrow_ref, rows_of(raw_ref), tiles, strip, margin)

    @pl.when(which >= slices - 2)
    def _():
        clear(mid, 5, tiles, (0, pad + window))
        widen(state, start_ref, window, tiles, pad)
        first_stage(state, mid, keep, range(total), pad, size, tiles)
        second_stage(state, mid, keep, range(total), pad, size, tiles, put_first)

        @pl.when(which == slices - 2)
        def _():
            copy_natural(narrow_ref, rows_of(state, pad), tiles, strip, BLOCK + margin)

        first_stage(state, mid, keep, range(total), pad, size, tiles)
        second_stage(state, mid, keep, range(1, total - 1), pad, size, tiles, put_second)

        @pl.when(which == slices - 1)
        def _():
            copy_natural(narrow_ref, rows_of(wide_ref), tiles, strip, margin)


def settle(raw, start, relaxed, coarse, keep, strip, margin, slices):
    tiles, wide = raw.shape[1:3]
    layout = (strip, margin, tiles, slices)
    padded = (5, tiles, wide + 4 * BLOCK, LANES)
    return call(
        lambda *refs: settle_kernel(layout, *refs),
        "settle",
        1,
        (array(3, strip, tiles * LANES), array(3, tiles, wide, LANES)),
        [raw, start, relaxed, coarse, keep],
        [scratch(*padded), scratch(*padded)],
    )


def inner(keep):
    return keep.at[:, pl.ds(BLOCK, keep.shape[1] - 2 * BLOCK), :]


def link_kernel(tiles, standing_at, wide_ref, keep, out_ref, state, mid):
    wide = wide_ref.shape[2]
    pad = BLOCK
    total = wide // BLOCK
    size = STEPS * time_step
    keep = inner(keep)
    clear(mid, 5, tiles, (0, pad + wide))

    def put(block, i, olds, news):
        for f in range(3):
            out_ref[f, i, pl.ds(BLOCK * block, BLOCK), :] = news[f]

    linked = standing_at[0] > 2

    @pl.when(linked)
    def _():
        widen(state, wide_ref, wide, tiles, pad)
        first_stage(state, mid, keep, range(total), pad, size, tiles)
        second_stage(state, mid, keep, range(total), pad, size, tiles, put)

    @pl.when(jnp.logical_not(linked))
    def _():
        copy_rows(out_ref, lambda f, i, row, take: wide_ref[f, i, pl.ds(row, take), :], tiles, wide, 0, 0)


def first_link(wide, keep):
    tiles, rows = wide.shape[1:3]
    padded = (5, tiles, rows + 2 * BLOCK, LANES)
    return call(
        lambda *refs: link_kernel(tiles, *refs),
        "first_link",
        1,
        (array(*wide.shape),),
        [wide, keep],
        [scratch(*padded), scratch(*padded)],
    )[0]


def last_kernel(layout, standing_at, start_ref, keep, far_ref, *refs):
    strip, margin, tiles, chain = layout
    more_refs = refs[:-4]
    c_ref, f_ref, state, mid = refs[-4:]
    wide = strip + 2 * margin
    pad = BLOCK
    which = standing_at[0]
    total = wide // BLOCK
    coarse_size = STEPS * time_step
    keep = inner(keep)

    clear(mid, 5, tiles, (0, pad + wide))

    def put(block, i, olds, news):
        store(state, i, pad + BLOCK * block, news)

    def add(defect, start_from):
        for f in range(3):
            for i in range(tiles):
                for b in range(0, wide - 4, BLOCK):
                    take = min(BLOCK, wide - 4 - b)
                    at = pl.ds(pad + 2 + b, take)
                    state[f, i, at, :] = start_from(f, i, 2 + b, take) + defect(f, i, b, take)
        for i in range(tiles):
            for b in range(0, wide, BLOCK):
                at = pl.ds(pad + b, BLOCK)
                height = 2.0 + state[0, i, at, :]
                state[3, i, at, :] = height * state[1, i, at, :]
                state[4, i, at, :] = height * state[2, i, at, :]

    def of_start(f, i, row, take):
        return start_ref[f, i, pl.ds(row, take), :]

    def of_state(f, i, row, take):
        return state[f, i, pl.ds(pad + row, take), :]

    def of_rows(ref):
        return lambda f, i, row, take: ref[f, i, pl.ds(row, take), :]

    def link(turn):
        if turn:
            first_stage(state, mid, keep, range(total), pad, coarse_size, tiles)
            second_stage(state, mid, keep, range(total), pad, coarse_size, tiles, put)
        defect = of_rows(more_refs[0].at[turn]) if more_refs else of_rows(far_ref)
        add(defect, of_state if turn else of_start)

    for turn in range(chain):
        pl.when(which > turn + 2)(lambda turn=turn: link(turn))
    pl.when(which <= 2)(lambda: widen(state, start_ref, wide, tiles, pad))

    first = margin // BLOCK
    strip_blocks = range(first, first + strip // BLOCK)

    early = which < 2

    def put_to(ref, value_of):
        def put_one(block, i, olds, news):
            at = pl.ds((block - first) * BLOCK, BLOCK)
            for f in range(3):
                value = value_of(f, i, at, news[f])
                ready[f].append(0.5 * value if f == 0 else value)
                if len(ready[f]) == tiles:
                    for p, natural in enumerate(gathered(ready[f])):
                        ref[f, at, pl.ds(p * LANES, LANES)] = natural
                    ready[f].clear()

        ready = [[], [], []]
        return put_one

    def c_value(f, i, at, new):
        return new

    def f_value(f, i, at, new):
        return jnp.where(early, far_ref[f, i, at, :], new)

    around = range(first - 1, first + strip // BLOCK + 1)
    first_stage(state, mid, keep, around, pad, coarse_size, tiles)
    second_stage(state, mid, keep, strip_blocks, pad, coarse_size, tiles, put_to(c_ref, c_value))

    def steps(blocks, group):
        def one(turn, carry):
            first_stage(state, mid, keep, blocks, pad, time_step, tiles)
            second_stage(state, mid, keep, blocks, pad, time_step, tiles, put)
            return carry

        if group > 0:
            lax.fori_loop(0, group, one, 0)

    near = min(BLOCK // 2 - 1, STEPS - 2)
    steps(range(total), STEPS - 2 - near)
    steps(around, near)
    first_stage(state, mid, keep, around, pad, time_step, tiles)
    second_stage(state, mid, keep, strip_blocks, pad, time_step, tiles, put_to(f_ref, f_value))


def last_chain(start, keep, far, more, strip, margin):
    tiles = start.shape[1]
    chain = more[0].shape[0] if more else 1
    layout = (strip, margin, tiles, chain)
    padded = (5, tiles, start.shape[2] + 2 * BLOCK, LANES)
    return call(
        lambda *refs: last_kernel(layout, *refs),
        "last_chain",
        3,
        (array(3, strip, tiles * LANES), array(3, strip, tiles * LANES)),
        [start, keep, far, *more],
        [scratch(*padded), scratch(*padded)],
    )


def finish_kernel(standing_at, coarse_ref, fine_ref, got_ref, c_ref, f_ref):
    early = standing_at[0] < 2
    strip, columns = coarse_ref.shape[1:]
    for f in range(3):
        for b in range(0, strip, BLOCK):
            for p in range(0, columns, LANES):
                at = (f, pl.ds(b, BLOCK), pl.ds(p, LANES))
                got = got_ref[at]
                c_ref[at] = jnp.where(early, got, coarse_ref[at] + got)
                f_ref[at] = fine_ref[at]


def finish(coarse, fine, got):
    out = array(*coarse.shape)
    return call(finish_kernel, "finish", 1, (out, out), [coarse, fine, got])


def body(initial_state, c_guess, friction):
    slices, strips = lax.axis_size("tm"), lax.axis_size("space")
    strip = initial_state.shape[1]
    which = lax.axis_index("tm")
    margin = 2 * (STEPS - 1) + 2 * (slices - 3)
    count = -(-(4 * STEPS + margin) // strip)
    both = ("tm", "space")

    def moved(value, target):
        pairs = []
        for t in range(slices):
            for s in range(strips):
                to = target(t, s)
                if to is not None:
                    pairs.append((t * strips + s, to[0] * strips + to[1] % strips))
        return lax.ppermute(value, both, pairs)

    place = lax.axis_index("space")
    paired = count == 2 and strips % 4 == 0
    side, turn = place % 2, place // 2 % 2
    start = jnp.where(which >= slices - 2, initial_state, c_guess[0])
    own = jnp.concatenate([start, friction[None]], axis=0)
    if paired:
        partner = moved(own, lambda t, s: (t, s ^ 1))
        one = moved(own, lambda t, s: (t, s ^ 2))
        other = moved(own, lambda t, s: (t, s - 2 if s // 2 % 2 == 0 else s + 2))
        relayed = moved(jnp.where(side == turn, one, other), lambda t, s: (t, s ^ 1))
        own, partner, one, other = deal(own, partner, one, other)
        parts = [one, relayed, own, partner, other]
    else:
        parts = []
        for offset in range(-count, count + 1):
            parts.append(own if offset == 0 else moved(own, lambda t, s, o=offset: (t, s - o)))
        parts = list(deal(*parts))
    far, raw, begin, relaxed, stepped, keep = fine_chain(parts, margin, slices, paired)

    got_far = moved(far, lambda t, s: (slices - 1 - t, s))
    narrow, wide = settle(raw, begin, relaxed, stepped, keep, strip, margin, slices)
    got = moved(narrow, lambda t, s: ((t + 2) % slices, s))
    more = []
    if slices != 4:
        everyone = lax.all_gather(wide, "tm", axis=0)
        more = [everyone[: slices - 3, :, :, 2:-2]]
        wide = everyone[slices - 1]
    first = first_link(wide, keep)
    coarse, fine = last_chain(first, keep, got_far, more, strip, margin)
    c_points, f_points = finish(coarse, fine, got)
    return (c_points[None], f_points[None])


def solution(mesh):
    placed = (P(None, "space", None), P("tm", None, "space", None), P("space", None))
    return jax.shard_map(
        body,
        mesh=mesh,
        in_specs=placed,
        out_specs=(P("tm", None, "space", None), P("tm", None, "space", None)),
        check_vma=False,
    )
```
